256 devices in a mesh: prow: 16 (over y, x_lo, core), pcol: 16 (over x_hi, z).
Axes of the slice: x: 4 (x_hi: 2, x_lo: 2; x = x_hi * 2 + x_lo), y: 4, z: 8, core: 2. Of those that a mesh axis runs over, the one named last changes fastest.
Arguments:
- ancestor_inverse: float32 [16, 16, 512, 512], P('prow', 'pcol'), may hold values from -0.0625 to 0.0625
- factor_panel: float32 [512, 16, 3, 512], P('pcol', 'prow'), may hold values from -0.75 to 0.75
- pivot_inverse: float32 [3, 512, 512], P(None, 'prow', 'pcol'), may hold values from -6 to 6
- structure: int32 [16, 3], replicated, may hold values from 0 to 1, as said below
Outputs:
- inverse_panel: float32 [512, 16, 3, 512], P('pcol', 'prow')
- diagonal_block: float32 [3, 512, 512], P(None, 'prow', 'pcol')
The draws below stay inside these ranges and needn't reach their ends.
Inputs may be any that keep to these rules, and one draw needn't show every extreme that they name: structure[J, K] is 1 where ancestor J lies in supernode K's structure and 0 elsewhere; the last ancestor, 15, lies in every supernode's structure.
All inputs are finite; a program needn't handle non-finite values.
Results may differ from the reference program's by a relative error of at most 0.00007.
Values sent between devices are 32-bit elements; how exact they have to be, the bound alone decides.
No kernel may reach another device: no remote copies, remote signals or barrier semaphores. Data moves between devices by JAX's collectives and lax.ppermute only.
A program may use at most 64 MiB of HBM per device.

```python
import jax
import jax.numpy as jnp
from jax import lax

B = 512
SUPER = 3
M = 16


def draw_structure(key, part):
    drawn_levels = jax.random.randint(key, (M, SUPER), 0, M)
    ancestor_index = jnp.arange(M, dtype=jnp.int32)[:, None]
    return jnp.where(drawn_levels <= ancestor_index, 1, 0).astype(jnp.int32)


def level_of(rng, extent, shards, smallest, largest):
    level = 1.0
    for position, shards_of in shards:
        draws = jax.random.uniform(jax.random.fold_in(jax.random.fold_in(rng, 6), position), (shards_of,), jnp.float32, smallest / len(shards), largest / len(shards))
        level = level * jnp.repeat(jnp.exp(draws), extent[position] // shards_of).reshape((-1,) + (1,) * (len(extent) - 1 - position))
    return level


def gaussian(rng, shape, scale, limit, pieces=(), held_as=jnp.bfloat16):
    factor_of = level_of(rng, shape, pieces, -0.22, 0.18) if pieces else 1.0
    values = jax.random.normal(rng, shape, jnp.float32) * scale * factor_of
    return jnp.minimum(jnp.maximum(values, -limit), limit).astype(held_as)


def setup_inputs(seed: int = 0) -> dict:
    keys = jax.random.split(jax.random.key(seed), 5)
    return {
        "ancestor_inverse": gaussian(keys[0], (M, M, B, B), (M * B) ** -0.5, 0.0625, ((0, 16), (1, 16)), jnp.float32),
        "factor_panel": gaussian(keys[1], (B, M, SUPER, B), 0.125, 0.75, ((0, 16), (1, 16)), jnp.float32),
        "pivot_inverse": gaussian(keys[2], (SUPER, B, B), 1.0, 6.0, ((1, 16), (2, 16)), jnp.float32),
        "structure": draw_structure(jax.random.fold_in(keys[4], 71), 0),
    }


def reference(ancestor_inverse, factor_panel, pivot_inverse, structure):
    struct_float = structure.astype(jnp.float32)
    masked = factor_panel * struct_float[None, :, :, None]

    def one_row(inverse_row):
        return jnp.einsum("Jrt,tJKc->rKc", inverse_row, masked, precision=lax.Precision.HIGHEST, preferred_element_type=jnp.float32)

    product = lax.map(one_row, ancestor_inverse)
    product = jnp.transpose(product, (1, 0, 2, 3))
    inverse_panel = -struct_float[None, :, :, None] * product
    diagonal_block = pivot_inverse - jnp.einsum("riKa,riKb->Kab", masked, inverse_panel, precision=lax.Precision.HIGHEST, preferred_element_type=jnp.float32)
    return inverse_panel, diagonal_block
```

```python
import jax
import jax.numpy as jnp
from jax import lax
from jax.sharding import Mesh
from jax.sharding import PartitionSpec as P

ALL = ("y", "xl", "c", "xh", "z")
SIZES = (4, 2, 2, 2, 8)
ROW = ("y", "xl", "c")
COL = ("xh", "z")
CHIPS = ("y", "xl")
SWAP = [(0, 1), (1, 0)]
UP = [(k, (k + 1) % 8) for k in range(8)]
DOWN = [(k, (k - 1) % 8) for k in range(8)]
HIGH = lax.Precision.HIGH
PARTS = 3


def pairs_of(target):
    pairs = []
    for d in range(256):
        z, xh, c, xl, y = d % 8, d // 8 % 2, d // 16 % 2, d // 32 % 2, d // 64
        y, xl, c, xh, z = target(y, xl, c, xh, z)
        pairs.append((d, (((y * 2 + xl) * 2 + c) * 2 + xh) * 8 + z))
    return pairs


def to_column(turn):
    def target(y, xl, c, xh, z):
        block, piece = (y * 2 + xl) * 2 + c, xh * 8 + z
        chip = piece // 2
        return chip // 2, chip % 2, turn ^ (piece % 2), block // 8, block % 8

    return target


def to_tile(y, xl, c, xh, z):
    rows = xh * 8 + z
    return rows // 4, rows // 2 % 2, rows % 2, c, y * 2 + xl


def send(value, target):
    return lax.ppermute(value, ALL, pairs_of(target))


def exchange(parts, axes):
    return lax.all_to_all(parts, axes, 0, 0, tiled=True)


def spread(piece):
    copies = jnp.broadcast_to(piece[None], (8, *piece.shape))
    return exchange(copies, CHIPS)


def up(value):
    return lax.ppermute(value, "z", UP)


def down(value):
    return lax.ppermute(value, "z", DOWN)


def ring_sum(parts):
    half = parts.shape[1] // 2
    ahead, behind = up(parts[4, :half]), down(parts[4, half:])
    ahead = up(jnp.concatenate([parts[3, :half] + ahead, parts[3, half:]]))
    behind = down(jnp.concatenate([parts[5, :half], parts[5, half:] + behind]))
    ahead, behind = up(parts[2] + ahead), down(parts[6] + behind)
    ahead, behind = up(parts[1] + ahead), down(parts[7] + behind)
    return parts[0] + ahead + behind


def body(ancestor_inverse, factor_panel, pivot_inverse, structure):
    row = lax.axis_index(ROW)
    core = lax.axis_index("c")
    z = lax.axis_index("z")
    xh = lax.axis_index("xh")
    struct_float = structure.astype(jnp.float32)
    own_mask = lax.dynamic_slice_in_dim(struct_float, row, 1, 0)[0]
    other_mask = lax.dynamic_slice_in_dim(struct_float, row ^ 1, 1, 0)[0]
    panel = factor_panel[:, 0] * own_mask[None, :, None]

    left, right = (panel[:, :, :256], panel[:, :, 256:])
    first = send(jnp.where(z % 2 == 0, left, right), to_column(0))
    second = send(jnp.where(z % 2 == 0, right, left), to_column(1))

    block = ancestor_inverse[0, 0].reshape(2, 8, 32, 512)
    block = jnp.where(xh == 0, block, block[::-1])
    block = lax.dynamic_slice_in_dim(jnp.concatenate([block, block], 1), z, 8, 1).transpose(1, 0, 2, 3)
    other = lax.ppermute(block, "c", SWAP)
    pair = jnp.stack([block, other], 2).reshape(1024, 512)

    even_rows = jnp.where(core == 0, first, second)
    odd_rows = jnp.where(core == 0, second, first)
    column_panel = spread(jnp.stack([even_rows, odd_rows]).reshape(64, 768)).reshape(512, 768)

    products = []
    step = 768 // PARTS
    for part in range(PARTS):
        columns = column_panel[:, part * step : (part + 1) * step]
        running = jnp.dot(pair, columns, precision=HIGH, preferred_element_type=jnp.float32)
        both = ring_sum(running.reshape(8, 128, step)).reshape(2, 64, step)
        products.append(both[0] + lax.ppermute(both[1], "xh", SWAP))
    product = jnp.concatenate(products, -1)
    masks = jnp.stack([own_mask, other_mask])
    inverse = -masks[:, None, :, None] * product.reshape(2, 32, 3, 256)

    got = lax.ppermute(inverse[1], "c", SWAP)
    inverse_panel = jnp.where(
        core == 0,
        jnp.concatenate([inverse[0], got], -1),
        jnp.concatenate([got, inverse[0]], -1),
    )

    left_own = spread(panel.reshape(32, 1536)).reshape(256, 1536)
    left_other = lax.ppermute(left_own, "c", SWAP)
    right_side = inverse.reshape(64, 3, 8, 32).transpose(2, 0, 1, 3).reshape(8, 64, 96)
    right_side = exchange(right_side, CHIPS).reshape(8, 2, 32, 96)
    full = 0
    for side, rows in ((left_own, right_side[:, 0]), (left_other, right_side[:, 1])):
        full = full + lax.dot_general(
            side,
            rows.reshape(256, 96),
            (((0,), (0,)), ((), ())),
            precision=HIGH,
            preferred_element_type=jnp.float32,
        )
    full = full.reshape(3, 512, 96)
    lane = lax.broadcasted_iota(jnp.int32, (512, 96), 1) // 32
    term = jnp.where(lane == 0, full[0], jnp.where(lane == 1, full[1], full[2]))
    tile = jnp.sum(exchange(term.reshape(16, 32, 96), COL), 0)
    tile = send(tile, to_tile)
    tile = tile.reshape(32, 3, 32).transpose(1, 0, 2)
    return (inverse_panel[:, None], pivot_inverse - tile)


def solution(mesh):
    torus = Mesh(mesh.devices.reshape(SIZES), ALL)
    return jax.shard_map(
        body,
        mesh=torus,
        in_specs=(P(ROW, COL, None, None), P(COL, ROW, None, None), P(None, ROW, COL), P()),
        out_specs=(P(COL, ROW, None, None), P(None, ROW, COL)),
        check_vma=False,
    )
```

```python
import jax
import jax.numpy as jnp
from jax import lax
from jax.sharding import Mesh
from jax.sharding import PartitionSpec as P

ALL = ("y", "xl", "c", "xh", "z")
SIZES = (4, 2, 2, 2, 8)
ROW = ("y", "xl", "c")
COL = ("xh", "z")
CHIPS = ("y", "xl")
SWAP = [(0, 1), (1, 0)]
UP = [(k, (k + 1) % 8) for k in range(8)]
DOWN = [(k, (k - 1) % 8) for k in range(8)]
HIGH = lax.Precision.HIGH
PARTS = 2


def pairs_of(target):
    pairs = []
    for d in range(256):
        z, xh, c, xl, y = d % 8, d // 8 % 2, d // 16 % 2, d // 32 % 2, d // 64
        y, xl, c, xh, z = target(y, xl, c, xh, z)
        pairs.append((d, (((y * 2 + xl) * 2 + c) * 2 + xh) * 8 + z))
    return pairs


def to_column(turn):
    def target(y, xl, c, xh, z):
        block, piece = (y * 2 + xl) * 2 + c, xh * 8 + z
        chip = piece // 2
        return chip // 2, chip % 2, turn ^ (piece % 2), block // 8, block % 8

    return target


def to_tile(y, xl, c, xh, z):
    rows = xh * 8 + z
    return rows // 4, rows // 2 % 2, rows % 2, c, y * 2 + xl


def send(value, target):
    return lax.ppermute(value, ALL, pairs_of(target))


def exchange(parts, axes):
    return lax.all_to_all(parts, axes, 0, 0, tiled=True)


def spread(piece):
    copies = jnp.broadcast_to(piece[None], (8, *piece.shape))
    return exchange(copies, CHIPS)


def up(value):
    return lax.ppermute(value, "z", UP)


def down(value):
    return lax.ppermute(value, "z", DOWN)


def ring_sum(parts):
    half = parts.shape[1] // 2
    ahead, behind = up(parts[4, :half]), down(parts[4, half:])
    ahead = up(jnp.concatenate([parts[3, :half] + ahead, parts[3, half:]]))
    behind = down(jnp.concatenate([parts[5, :half], parts[5, half:] + behind]))
    ahead, behind = up(parts[2] + ahead), down(parts[6] + behind)
    ahead, behind = up(parts[1] + ahead), down(parts[7] + behind)
    return parts[0] + ahead + behind


def body(ancestor_inverse, factor_panel, pivot_inverse, structure):
    row = lax.axis_index(ROW)
    core = lax.axis_index("c")
    z = lax.axis_index("z")
    xh = lax.axis_index("xh")
    own_mask = lax.dynamic_slice_in_dim(structure, row, 1, 0)[0].astype(jnp.float32)
    other_mask = lax.dynamic_slice_in_dim(structure, row ^ 1, 1, 0)[0].astype(jnp.float32)
    panel = factor_panel[:, 0] * own_mask[None, :, None]

    left, right = (panel[:, :, :256], panel[:, :, 256:])
    first = send(jnp.where(z % 2 == 0, left, right), to_column(0))
    second = send(jnp.where(z % 2 == 0, right, left), to_column(1))

    block = ancestor_inverse[0, 0].reshape(2, 8, 32, 512)
    block = jnp.where(xh == 0, block, block[::-1])
    block = lax.dynamic_slice_in_dim(jnp.concatenate([block, block], 1), z, 8, 1).transpose(1, 0, 2, 3)
    other = lax.ppermute(block, "c", SWAP)
    pair = jnp.stack([block, other], 2).reshape(1024, 512)

    even_rows = jnp.where(core == 0, first, second)
    odd_rows = jnp.where(core == 0, second, first)
    piece = jnp.stack([even_rows, odd_rows]).reshape(64, 768)

    column_panel = spread(piece).reshape(512, 768)
    own_rows = panel.reshape(32, 1536)
    column_panel, own_rows = lax.optimization_barrier((column_panel, own_rows))

    products = []
    step = 768 // PARTS
    for part in range(PARTS):
        columns = column_panel[:, part * step : (part + 1) * step]
        running = jnp.dot(pair, columns, precision=HIGH, preferred_element_type=jnp.float32)
        both = ring_sum(running.reshape(8, 128, step)).reshape(2, 64, step)
        products.append(both[0] + lax.ppermute(both[1], "xh", SWAP))
    product = jnp.concatenate(products, -1)
    masks = jnp.stack([own_mask, other_mask])
    inverse = -masks[:, None, :, None] * product.reshape(2, 32, 3, 256)

    got = lax.ppermute(inverse[1], "c", SWAP)
    inverse_panel = jnp.where(
        core == 0,
        jnp.concatenate([inverse[0], got], -1),
        jnp.concatenate([got, inverse[0]], -1),
    )

    left_own = spread(own_rows).reshape(256, 1536)
    left_other = lax.ppermute(left_own, "c", SWAP)
    right_side = inverse.reshape(64, 3, 8, 32).transpose(2, 0, 1, 3).reshape(8, 64, 96)
    right_side = exchange(right_side, CHIPS).reshape(8, 2, 32, 96)
    full = 0
    for side, rows in ((left_own, right_side[:, 0]), (left_other, right_side[:, 1])):
        full = full + lax.dot_general(
            side,
            rows.reshape(256, 96),
            (((0,), (0,)), ((), ())),
            precision=HIGH,
            preferred_element_type=jnp.float32,
        )
    full = full.reshape(3, 512, 96)
    lane = lax.broadcasted_iota(jnp.int32, (512, 96), 1) // 32
    term = jnp.where(lane == 0, full[0], jnp.where(lane == 1, full[1], full[2]))
    tile = jnp.sum(exchange(term.reshape(16, 32, 96), COL), 0)
    tile = send(tile, to_tile)
    tile = tile.reshape(32, 3, 32).transpose(1, 0, 2)
    return (inverse_panel[:, None], pivot_inverse - tile)


def solution(mesh):
    torus = Mesh(mesh.devices.reshape(SIZES), ALL)
    return jax.shard_map(
        body,
        mesh=torus,
        in_specs=(P(ROW, COL, None, None), P(COL, ROW, None, None), P(None, ROW, COL), P()),
        out_specs=(P(COL, ROW, None, None), P(None, ROW, COL)),
        check_vma=False,
    )
```

```python
import jax
import jax.numpy as jnp
from jax import lax
from jax.sharding import Mesh
from jax.sharding import PartitionSpec as P

ALL = ("y", "xl", "c", "xh", "z")
SIZES = (4, 2, 2, 2, 8)
ROW = ("y", "xl", "c")
COL = ("xh", "z")
CHIPS = ("y", "xl")
SWAP = [(0, 1), (1, 0)]
UP = [(k, (k + 1) % 8) for k in range(8)]
DOWN = [(k, (k - 1) % 8) for k in range(8)]
HIGH = lax.Precision.HIGH
PARTS = 2


def pairs_of(target):
    pairs = []
    for d in range(256):
        z, xh, c, xl, y = d % 8, d // 8 % 2, d // 16 % 2, d // 32 % 2, d // 64
        y, xl, c, xh, z = target(y, xl, c, xh, z)
        pairs.append((d, (((y * 2 + xl) * 2 + c) * 2 + xh) * 8 + z))
    return pairs


def to_column(turn):
    def target(y, xl, c, xh, z):
        block, piece = (y * 2 + xl) * 2 + c, xh * 8 + z
        chip = piece // 2
        return chip // 2, chip % 2, turn ^ (piece % 2), block // 8, block % 8

    return target


def to_tile(y, xl, c, xh, z):
    rows = xh * 8 + z
    return rows // 4, rows // 2 % 2, rows % 2, c, y * 2 + xl


def send(value, target):
    return lax.ppermute(value, ALL, pairs_of(target))


def exchange(parts, axes):
    return lax.all_to_all(parts, axes, 0, 0, tiled=True)


def spread(piece):
    copies = jnp.broadcast_to(piece[None], (8, *piece.shape))
    return exchange(copies, CHIPS)


def up(value):
    return lax.ppermute(value, "z", UP)


def down(value):
    return lax.ppermute(value, "z", DOWN)


def ring_sum(parts):
    half = parts.shape[1] // 2
    ahead, behind = up(parts[4, :half]), down(parts[4, half:])
    ahead = up(jnp.concatenate([parts[3, :half] + ahead, parts[3, half:]]))
    behind = down(jnp.concatenate([parts[5, :half], parts[5, half:] + behind]))
    ahead, behind = up(parts[2] + ahead), down(parts[6] + behind)
    ahead, behind = up(parts[1] + ahead), down(parts[7] + behind)
    return parts[0] + ahead + behind


def body(ancestor_inverse, factor_panel, pivot_inverse, structure):
    row = lax.axis_index(ROW)
    core = lax.axis_index("c")
    z = lax.axis_index("z")
    xh = lax.axis_index("xh")
    own_mask = lax.dynamic_slice_in_dim(structure, row, 1, 0)[0].astype(jnp.float32)
    other_mask = lax.dynamic_slice_in_dim(structure, row ^ 1, 1, 0)[0].astype(jnp.float32)
    column_mask = lax.dynamic_slice_in_dim(structure, lax.axis_index(COL), 1, 0)[0].astype(jnp.float32)
    panel = factor_panel[:, 0]

    left, right = (panel[:, :, :256], panel[:, :, 256:])
    first = send(jnp.where(z % 2 == 0, left, right), to_column(0))
    second = send(jnp.where(z % 2 == 0, right, left), to_column(1))

    block = ancestor_inverse[0, 0].reshape(2, 8, 32, 512)
    block = jnp.where(xh == 0, block, block[::-1])
    block = lax.dynamic_slice_in_dim(jnp.concatenate([block, block], 1), z, 8, 1).transpose(1, 0, 2, 3)
    other = lax.ppermute(block, "c", SWAP)
    pair = jnp.stack([block, other], 2).reshape(1024, 512)

    even_rows = jnp.where(core == 0, first, second)
    odd_rows = jnp.where(core == 0, second, first)
    piece = (jnp.stack([even_rows, odd_rows]) * column_mask[None, None, :, None]).reshape(64, 768)

    column_panel = spread(piece).reshape(512, 768)
    own_rows = panel.reshape(32, 1536)
    column_panel, own_rows = lax.optimization_barrier((column_panel, own_rows))

    products = []
    step = 768 // PARTS
    for part in range(PARTS):
        columns = column_panel[:, part * step : (part + 1) * step]
        running = jnp.dot(pair, columns, precision=HIGH, preferred_element_type=jnp.float32)
        both = ring_sum(running.reshape(8, 128, step)).reshape(2, 64, step)
        products.append(both[0] + lax.ppermute(both[1], "xh", SWAP))
    product = jnp.concatenate(products, -1)
    masks = jnp.stack([own_mask, other_mask])
    inverse = -masks[:, None, :, None] * product.reshape(2, 32, 3, 256)

    got = lax.ppermute(inverse[1], "c", SWAP)
    inverse_panel = jnp.where(
        core == 0,
        jnp.concatenate([inverse[0], got], -1),
        jnp.concatenate([got, inverse[0]], -1),
    )

    left_own = spread(own_rows).reshape(256, 1536)
    left_other = lax.ppermute(left_own, "c", SWAP)
    right_side = inverse.reshape(64, 3, 8, 32).transpose(2, 0, 1, 3).reshape(8, 64, 96)
    right_side = exchange(right_side, CHIPS).reshape(8, 2, 32, 96)
    full = 0
    for side, rows in ((left_own, right_side[:, 0]), (left_other, right_side[:, 1])):
        full = full + lax.dot_general(
            side,
            rows.reshape(256, 96),
            (((0,), (0,)), ((), ())),
            precision=HIGH,
            preferred_element_type=jnp.float32,
        )
    full = full.reshape(3, 512, 96)
    lane = lax.broadcasted_iota(jnp.int32, (512, 96), 1) // 32
    term = jnp.where(lane == 0, full[0], jnp.where(lane == 1, full[1], full[2]))
    tile = jnp.sum(exchange(term.reshape(16, 32, 96), COL), 0)
    tile = send(tile, to_tile)
    tile = tile.reshape(32, 3, 32).transpose(1, 0, 2)
    return (inverse_panel[:, None], pivot_inverse - tile)


def solution(mesh):
    torus = Mesh(mesh.devices.reshape(SIZES), ALL)
    return jax.shard_map(
        body,
        mesh=torus,
        in_specs=(P(ROW, COL, None, None), P(COL, ROW, None, None), P(None, ROW, COL), P()),
        out_specs=(P(COL, ROW, None, None), P(None, ROW, COL)),
        check_vma=False,
    )
```
